64 devices in a mesh: dp: 4 (over x, y), ep: 16 (over z, core).
Axes of the slice: x: 2, y: 2, z: 8, core: 2. Of those that a mesh axis runs over, the one named last changes fastest.
The devices are a block of a 4x4x8 slice.
Arguments:
- hidden: bfloat16 [65536, 4096], P(('dp', 'ep')), parts along dimension 0
- ln_gamma: float32 [4096], replicated
- ln_beta: float32 [4096], replicated
- w_router: bfloat16 [4096, 16], replicated
- w_gate: bfloat16 [16, 4096, 448], P('ep')
- w_up: bfloat16 [16, 4096, 448], P('ep')
- w_down: bfloat16 [16, 448, 4096], P('ep')
- choice: int32 [65536, 2], P(('dp', 'ep')), parts along dimension 0
- mask_first: int32 [65536, 16], P(('dp', 'ep')), parts along dimension 0
- mask_second: int32 [65536, 16], P(('dp', 'ep')), parts along dimension 0
Outputs:
- output: bfloat16 [65536, 4096], P(('dp', 'ep')), parts along dimension 0
There are 4 independent parts. The reference program is written for one: setup_inputs(seed, part) draws one part's arguments, and reference() takes and returns one part's arrays. A program takes and returns all parts, laid end to end along the dimension named above; an argument that names none is the same for every part.
All inputs are finite; a program needn't handle non-finite values.
Results may differ from the reference program's by a relative error of at most 0.001.
Values are sent between devices in bfloat16 or wider.
A program may use at most 768 MiB of HBM per device.

```python
import jax
import jax.numpy as jnp
from jax import lax

D_MODEL = 4096
FF_WIDTH = 448
EXPERTS = 16
TOKENS_DEV = 1024
GROUP_DEVS = 16
TOKENS = GROUP_DEVS * TOKENS_DEV
CAPACITY = (10 * TOKENS_DEV + 4 * EXPERTS - 1) // (4 * EXPERTS)
LN_EPS = 1e-5


def draw_routing(route_key):
    sub_keys = jax.random.split(route_key, 6)
    favoured = jax.random.randint(sub_keys[0], (), 0, EXPERTS)
    coin_flip = jax.random.randint(sub_keys[1], (TOKENS,), 0, 4)
    spread = jax.random.randint(sub_keys[2], (TOKENS,), 0, EXPERTS)
    first_pick = jnp.where(coin_flip == 0, favoured, spread)
    second_pick = (first_pick + 1 + jax.random.randint(sub_keys[3], (TOKENS,), 0, EXPERTS - 1)) % EXPERTS
    expert_ids = jnp.arange(EXPERTS)
    is_first = first_pick[:, None] == expert_ids
    is_second = second_pick[:, None] == expert_ids
    keep_first = jax.random.randint(sub_keys[4], (TOKENS, EXPERTS), 0, 4) == 0
    keep_second = jax.random.randint(sub_keys[5], (TOKENS, EXPERTS), 0, 4) == 0
    mask_first = (keep_first | is_first).astype(jnp.int32)
    mask_second = ((keep_second | is_second) & (~is_first)).astype(jnp.int32)
    choice = jnp.stack([first_pick, second_pick], axis=1).astype(jnp.int32)
    return choice, mask_first, mask_second


def setup_inputs(seed: int = 0, part: int = 0) -> dict:
    shared_keys = jax.random.split(jax.random.key(seed), 6)
    part_keys = jax.random.split(jax.random.fold_in(jax.random.key(seed + 1), part), 2)
    hidden = jax.random.normal(part_keys[0], (TOKENS, D_MODEL), jnp.float32).astype(jnp.bfloat16)
    choice, mask_first, mask_second = draw_routing(part_keys[1])
    ln_gamma = 1.0 + 0.4 * jax.random.normal(shared_keys[0], (D_MODEL,), jnp.float32)
    ln_beta = 0.4 * jax.random.normal(shared_keys[1], (D_MODEL,), jnp.float32)
    w_router = (jax.random.normal(shared_keys[2], (D_MODEL, EXPERTS), jnp.float32) * D_MODEL ** -0.5).astype(jnp.bfloat16)
    w_gate = (jax.random.normal(shared_keys[3], (EXPERTS, D_MODEL, FF_WIDTH), jnp.float32) * D_MODEL ** -0.5).astype(jnp.bfloat16)
    w_up = (jax.random.normal(shared_keys[4], (EXPERTS, D_MODEL, FF_WIDTH), jnp.float32) * D_MODEL ** -0.5).astype(jnp.bfloat16)
    w_down = (jax.random.normal(shared_keys[5], (EXPERTS, FF_WIDTH, D_MODEL), jnp.float32) * FF_WIDTH ** -0.5).astype(jnp.bfloat16)
    return {"hidden": hidden, "ln_gamma": ln_gamma, "ln_beta": ln_beta, "w_router": w_router,
            "w_gate": w_gate, "w_up": w_up, "w_down": w_down, "choice": choice,
            "mask_first": mask_first, "mask_second": mask_second}


def layer_norm(token_rows, ln_gamma, ln_beta):
    values = token_rows.astype(jnp.float32)
    centred = values - jnp.mean(values, axis=-1, keepdims=True)
    variance = jnp.mean(centred * centred, axis=-1, keepdims=True)
    return (centred * lax.rsqrt(variance + LN_EPS) * ln_gamma + ln_beta).astype(jnp.bfloat16)


def reference(hidden, ln_gamma, ln_beta, w_router, w_gate, w_up, w_down, choice, mask_first, mask_second):
    normed = layer_norm(hidden, ln_gamma, ln_beta)
    scores = jnp.dot(normed, w_router, preferred_element_type=jnp.float32)
    mask_pair = jnp.stack([mask_first, mask_second], axis=1) > 0
    soft_probs = jax.nn.softmax(jnp.where(mask_pair, scores[:, None, :], -jnp.inf), axis=-1)
    gate_vals = jnp.take_along_axis(soft_probs, choice[:, :, None], axis=-1)[:, :, 0]
    by_source = choice.reshape(GROUP_DEVS, TOKENS_DEV, 2)
    expert_ids = jnp.arange(EXPERTS, dtype=jnp.int32)
    hit_count = (by_source[..., None] == expert_ids).astype(jnp.int32)
    per_token = jnp.sum(hit_count, axis=2)
    before = jnp.cumsum(per_token, axis=1) - per_token
    position = jnp.take_along_axis(before, by_source, axis=2)
    kept_copy = position < CAPACITY
    source_ids = jnp.broadcast_to(jnp.arange(GROUP_DEVS, dtype=jnp.int32)[:, None, None], by_source.shape)
    token_ids = jnp.broadcast_to(jnp.arange(TOKENS, dtype=jnp.int32).reshape(GROUP_DEVS, TOKENS_DEV, 1), by_source.shape)
    slot_table = jnp.zeros((EXPERTS, GROUP_DEVS, CAPACITY), jnp.int32)
    slot_table = slot_table.at[by_source, source_ids, position].set(token_ids, mode="drop")

    def one_expert(operands):
        row_index, gate_mat, up_mat, down_mat = operands
        expert_rows = normed[row_index.reshape(-1)]
        gate_proj = jnp.dot(expert_rows, gate_mat, preferred_element_type=jnp.float32)
        up_proj = jnp.dot(expert_rows, up_mat, preferred_element_type=jnp.float32)
        inner_act = (jax.nn.silu(gate_proj) * up_proj).astype(jnp.bfloat16)
        return jnp.dot(inner_act, down_mat, preferred_element_type=jnp.float32).astype(jnp.bfloat16)

    expert_out = lax.map(one_expert, (slot_table, w_gate, w_up, w_down))
    expert_out = expert_out.reshape(EXPERTS, GROUP_DEVS, CAPACITY, D_MODEL)
    picked = expert_out[by_source, source_ids, jnp.minimum(position, CAPACITY - 1)]
    kept_gates = jnp.where(kept_copy, gate_vals.reshape(GROUP_DEVS, TOKENS_DEV, 2), 0.0)
    mixed_out = hidden.reshape(GROUP_DEVS, TOKENS_DEV, D_MODEL).astype(jnp.float32) + jnp.sum(kept_gates[..., None] * picked.astype(jnp.float32), axis=2)
    return mixed_out.reshape(TOKENS, D_MODEL).astype(jnp.bfloat16)
```

```python
import functools
import math

import jax
import jax.numpy as jnp
from jax import lax
from jax.experimental import pallas as pl
from jax.experimental.pallas import tpu as pltpu
from jax.sharding import PartitionSpec as P

LN_EPS = 1e-5
LANES = 128
PARTS = 16
DEPTH = 4
MESH = pl.DeviceIdType.MESH


def moe_kernel(sizes, hidden_ref, gamma_ref, beta_ref, router_ref, gu_ref, wd_ref, choice_ref, first_ref, second_ref,
               out_ref, gu_all, wd_all,
               normed, total, gu_buf, wd_buf, row_buf, inner_buf, gate_table, gate_wide,
               ring_send, ring_recv, side_send, side_recv, pair_send, pair_recv, own_send, own_recv,
               row_sem, load_sem):
    ring, columns, capacity = sizes
    tokens, width = hidden_ref.shape
    ff = wd_ref.shape[0]
    experts = gu_all.shape[0]
    half = tokens // 2
    tile = tokens // 8
    part_rows = width // PARTS
    rounds = 4 * (ring - 1)
    dp = lax.axis_index("dp")
    ep = lax.axis_index("ep")
    z, core = ep // 2, ep % 2
    x, y = dp // columns, dp % columns
    parity = (x + y) % 2
    after, before = ((z + 1) % ring) * 2 + core, ((z + ring - 1) % ring) * 2 + core
    partner = z * 2 + 1 - core
    x_peer = (x + 1 - 2 * (x % 2)) * columns + y
    y_peer = x * columns + y + 1 - 2 * (y % 2)
    places = ((dp, after), (dp, before), (x_peer, ep), (y_peer, ep), (dp, partner))

    barrier = pltpu.get_barrier_semaphore()
    for place in places:
        pl.semaphore_signal(barrier, inc=1, device_id=place, device_id_type=MESH)
    pl.semaphore_wait(barrier, len(places))

    def pieces(gu_source, wd_source, expert, part):
        rows = pl.ds(pl.multiple_of(part * part_rows, part_rows), part_rows)
        gu_to, wd_to = gu_all.at[expert, rows, :], wd_all.at[expert, :, rows]
        if gu_source is None:
            return (gu_to, gu_to), (wd_to, wd_to)
        return (gu_source.at[rows, :], gu_to), (wd_source.at[:, rows], wd_to)

    def copies(both, send, recv, place):
        return [pltpu.make_async_remote_copy(src_ref=src, dst_ref=dst, send_sem=send.at[kind], recv_sem=recv.at[kind],
                                             device_id=place, device_id_type=MESH)
                for kind, (src, dst) in enumerate(both)]

    def ring_part(flow, index):
        return (index + 4 * flow) % 8

    def ring_copy(flow, index, own):
        expert = ((z + (index // 8) * (2 * flow - 1) + ring) % ring) * 2 + core
        part = 8 * parity + ring_part(flow, index)
        both = pieces(gu_ref if own else None, wd_ref if own else None, expert, part)
        return copies(both, ring_send.at[flow, index], ring_recv.at[flow, index], places[flow])

    def came(flow, index, of_core, of_parity):
        expert = ((z + (1 + index // 8) * (2 * flow - 1) + ring) % ring) * 2 + of_core
        return pieces(None, None, expert, 8 * of_parity + ring_part(flow, index))

    def ring_arrival(flow, index):
        return copies(came(flow, index, core, parity), ring_send.at[flow, index], ring_recv.at[flow, index], places[flow])

    def side_copy(flow, index, of_parity):
        carried = (index // 4 + flow) % 2
        return copies(came(carried, index, core, of_parity), side_send.at[flow, index], side_recv.at[flow, index],
                      places[2 + flow])

    def pair_copy(flow, index, of_core):
        if flow < 2:
            both = came(flow, index, of_core, parity)
        else:
            both = came((index // 4 + flow) % 2, index, of_core, 1 - parity)
        return copies(both, pair_send.at[flow, index], pair_recv.at[flow, index], places[4])

    def own_copy(expert):
        return copies(((gu_ref, gu_all.at[expert]), (wd_ref, wd_all.at[expert])), own_send, own_recv, places[4])

    def start(group):
        for copy in group:
            copy.start()

    def wait_recv(group):
        for copy in group:
            copy.wait_recv()

    def wait_send(group):
        for copy in group:
            copy.wait_send()

    def row_load(index):
        rows = pl.ds(pl.multiple_of(index * tile, tile), tile)
        return pltpu.make_async_copy(hidden_ref.at[rows, :], row_buf.at[index % 4], row_sem.at[index % 4])

    def expert_of(turn):
        place = (turn + 2) % 4
        return ((z + ((turn + 2) // 4) * (2 * (place // 2) - 1) + ring) % ring) * 2 + core + (place % 2) * (1 - 2 * core)

    def loads(gu_source, wd_source, slot):
        return (pltpu.make_async_copy(gu_source, gu_buf.at[slot], load_sem.at[slot, 0]),
                pltpu.make_async_copy(wd_source, wd_buf.at[slot, pl.ds(0, ff), :], load_sem.at[slot, 1]))

    def expert_loads(turn):
        expert = expert_of(turn)
        return loads(gu_all.at[expert], wd_all.at[expert], turn % 2)

    start(loads(gu_ref, wd_ref, 0))
    for index in range(4):
        row_load(index).start()
    for index in range(DEPTH):
        for flow in range(2):
            start(ring_copy(flow, index, True))
    start(own_copy(ep))
    padded = wd_buf.shape[1]
    wd_buf[:, pl.ds(ff, padded - ff), :] = jnp.zeros((2, padded - ff, width), wd_buf.dtype)

    def norm_tile(index):
        row_load(index).wait()
        rows = pl.ds(pl.multiple_of(index * tile, tile), tile)
        values = row_buf[index % 4].astype(jnp.float32)
        total[rows, :] = values
        centred = values - jnp.mean(values, axis=-1, keepdims=True)
        variance = jnp.mean(centred * centred, axis=-1, keepdims=True)
        normed[rows, :] = (centred * lax.rsqrt(variance + LN_EPS) * gamma_ref[...] + beta_ref[...]).astype(jnp.bfloat16)

        @pl.when(index + 4 < 8)
        def _():
            row_load(index + 4).start()

    def hits(rows, pick, count):
        ids = lax.broadcasted_iota(jnp.int32, (count, experts), 1)
        return ids == choice_ref[rows, pl.ds(pick, 1)]

    def gate_tile(index):
        step = 2 * tile
        rows = pl.ds(pl.multiple_of(index * step, step), step)
        scores = jnp.dot(normed[rows, :], router_ref[...], preferred_element_type=jnp.float32)
        every = pl.ds(0, tokens)
        per_token = sum(jnp.where(hits(every, pick, tokens), 1.0, 0.0) for pick in range(2)).astype(jnp.bfloat16)
        earlier = (lax.broadcasted_iota(jnp.int32, (step, tokens), 1)
                   < lax.broadcasted_iota(jnp.int32, (step, tokens), 0) + index * step)
        position = jnp.dot(jnp.where(earlier, 1.0, 0.0).astype(jnp.bfloat16), per_token, preferred_element_type=jnp.float32)
        table = jnp.full((step, experts), -1.0, jnp.float32)
        for pick, mask_ref in enumerate((first_ref, second_ref)):
            hit = hits(rows, pick, step)
            masked = jnp.where(mask_ref[rows, :] > 0, scores, -jnp.inf)
            powers = jnp.exp(masked - jnp.max(masked, axis=-1, keepdims=True))
            probs = powers / jnp.sum(powers, axis=-1, keepdims=True)
            table = jnp.where(hit & (position < capacity), probs, table)
        gate_table[rows, :] = table

    def expert_unit(unit):
        turn, part = unit // 2, unit % 2
        slot = turn % 2
        expert = expert_of(turn)

        @pl.when(part == 0)
        def _():
            for copy in expert_loads(turn):
                copy.wait()

        @pl.when((part == 1) & (turn == 0))
        def _():
            wait_recv(own_copy(partner))

        @pl.when((part == 1) & (turn + 1 < experts))
        def _():
            start(expert_loads(turn + 1))

        rows = pl.ds(pl.multiple_of(part * half, half), half)
        ids = lax.broadcasted_iota(jnp.int32, (half, experts), 1)
        gates = jnp.sum(jnp.where(ids == expert, gate_table[rows, :], 0.0), axis=-1, keepdims=True)
        gate_wide[...] = jnp.broadcast_to(gates, gate_wide.shape)

        def inner_tile(index, _):
            lanes = pl.ds(pl.multiple_of(index * 2 * LANES, 2 * LANES), 2 * LANES)
            both = jnp.dot(normed[rows, :], gu_buf[slot, :, lanes], preferred_element_type=jnp.float32)
            value = jax.nn.silu(both[:, :LANES]) * both[:, LANES:]
            inner_buf[:, pl.ds(pl.multiple_of(index * LANES, LANES), LANES)] = value.astype(jnp.bfloat16)
            return 0

        full = ff // LANES
        lax.fori_loop(0, full, inner_tile, 0)
        rest = ff - full * LANES
        both = jnp.dot(normed[rows, :], gu_buf[slot, :, pl.ds(full * 2 * LANES, LANES)], preferred_element_type=jnp.float32)
        value = jax.nn.silu(both) * pltpu.roll(both, LANES - rest, 1)
        lane = lax.broadcasted_iota(jnp.int32, value.shape, 1)
        inner_buf[:, pl.ds(full * LANES, LANES)] = jnp.where(lane < rest, value, 0.0).astype(jnp.bfloat16)

        step = width // PARTS

        def out_tile(index, _):
            lanes = pl.ds(pl.multiple_of(index * step, step), step)
            made = jnp.dot(inner_buf[...], wd_buf[slot, :, lanes], preferred_element_type=jnp.float32)
            made = made.astype(jnp.bfloat16).astype(jnp.float32)
            gate = jnp.concatenate([gate_wide[...]] * (step // LANES), axis=1) if step > LANES else gate_wide[:, :step]
            total[rows, lanes] += jnp.where(gate >= 0.0, gate * made, 0.0)
            return 0

        lax.fori_loop(0, PARTS, out_tile, 0)

    first_double = 4 * ring - 7

    def begin(step):
        return jnp.maximum(step - 5, 0) + jnp.maximum(step - first_double, 0)

    def step_body(step, _):
        @pl.when(step < rounds)
        def _():
            for flow in range(2):
                wait_recv(ring_arrival(flow, step))
            ahead = step + DEPTH
            for flow in range(2):
                @pl.when(ahead < 8)
                def _():
                    start(ring_copy(flow, ahead, True))

                @pl.when((ahead >= 8) & (ahead < rounds))
                def _():
                    start(ring_copy(flow, ahead, False))
            for flow in range(2):
                start(side_copy(flow, step, parity))
            for flow in range(2):
                start(pair_copy(flow, step, core))

        @pl.when((step >= 1) & (step <= rounds))
        def _():
            for flow in range(2):
                wait_recv(side_copy(flow, step - 1, 1 - parity))
            for flow in range(2):
                start(pair_copy(2 + flow, step - 1, core))

        @pl.when(step >= 2)
        def _():
            for flow in range(4):
                wait_recv(pair_copy(flow, step - 2, 1 - core))

        @pl.when(step < 4)
        def _():
            norm_tile(2 * step)
            norm_tile(2 * step + 1)

        @pl.when(step == 4)
        def _():
            lax.fori_loop(0, 4, lambda index, _: (gate_tile(index), 0)[1], 0)

        low = begin(step)
        high = jnp.where(step == rounds + 1, 2 * experts, begin(step + 1))
        lax.fori_loop(low, high, lambda unit, _: (expert_unit(unit), 0)[1], 0)
        return 0

    lax.fori_loop(0, rounds + 2, step_body, 0)

    def row_store(index):
        rows = pl.ds(pl.multiple_of(index * tile, tile), tile)
        return pltpu.make_async_copy(row_buf.at[index % 4], out_ref.at[rows, :], row_sem.at[index % 4])

    def store_tile(index, _):
        @pl.when(index >= 4)
        def _():
            row_store(index - 4).wait()
        rows = pl.ds(pl.multiple_of(index * tile, tile), tile)
        row_buf[index % 4] = total[rows, :].astype(row_buf.dtype)
        row_store(index).start()
        return 0

    lax.fori_loop(0, 8, store_tile, 0)
    for index in range(4, 8):
        row_store(index).wait()

    def finish(index, _):
        for flow in range(2):
            wait_send(ring_copy(flow, index, False))
            wait_send(side_copy(flow, index, parity))
        for flow in range(4):
            wait_send(pair_copy(flow, index, core))
        return 0

    lax.fori_loop(0, rounds, finish, 0)
    wait_send(own_copy(ep))


def pack_gate_up(w_gate, w_up):
    ff = w_gate.shape[1]
    full = ff // LANES
    pieces = []
    for index in range(full + 1):
        low, high = index * LANES, min(ff, (index + 1) * LANES)
        pieces += [w_gate[:, low:high], w_up[:, low:high]]
    return jnp.concatenate(pieces, axis=1)


def solution(mesh):
    group_size = mesh.shape["ep"]
    columns = math.isqrt(mesh.shape["dp"])
    rows_spec = P(("dp", "ep"))

    def device_step(hidden, ln_gamma, ln_beta, w_router, w_gate, w_up, w_down, choice, mask_first, mask_second):
        tokens, width = hidden.shape
        experts = w_gate.shape[0] * group_size
        ff = w_gate.shape[2]
        capacity = (10 * tokens + 4 * experts - 1) // (4 * experts)
        ring = group_size // 2
        rounds = 4 * (ring - 1)
        padded = -(-ff // LANES) * LANES
        packed = pack_gate_up(w_gate[0], w_up[0])
        dma = pltpu.SemaphoreType.DMA
        whole = pl.BlockSpec(memory_space=pl.ANY)
        local = pl.BlockSpec(memory_space=pltpu.VMEM)
        out, _, _ = pl.pallas_call(
            functools.partial(moe_kernel, (ring, columns, capacity)),
            out_shape=(jax.ShapeDtypeStruct(hidden.shape, hidden.dtype),
                       jax.ShapeDtypeStruct((experts, width, 2 * ff), w_gate.dtype),
                       jax.ShapeDtypeStruct((experts, ff, width), w_down.dtype)),
            in_specs=[whole, local, local, local, whole, whole, local, local, local],
            out_specs=(whole, whole, whole),
            scratch_shapes=[
                pltpu.VMEM((tokens, width), jnp.bfloat16),
                pltpu.VMEM((tokens, width), jnp.float32),
                pltpu.VMEM((2, width, 2 * ff), w_gate.dtype),
                pltpu.VMEM((2, padded, width), w_down.dtype),
                pltpu.VMEM((4, tokens // 8, width), hidden.dtype),
                pltpu.VMEM((tokens // 2, padded), jnp.bfloat16),
                pltpu.VMEM((tokens, experts), jnp.float32),
                pltpu.VMEM((tokens // 2, LANES), jnp.float32),
                dma((2, rounds, 2)), dma((2, rounds, 2)),
                dma((2, rounds, 2)), dma((2, rounds, 2)),
                dma((4, rounds, 2)), dma((4, rounds, 2)),
                dma((2,)), dma((2,)),
                dma((4,)), dma((2, 2)),
            ],
            compiler_params=pltpu.CompilerParams(collective_id=0, has_side_effects=True, vmem_limit_bytes=67043328),
            name="moe",
        )(hidden, ln_gamma.reshape(1, width), ln_beta.reshape(1, width), w_router, packed, w_down[0],
          choice, mask_first, mask_second)
        return out

    return jax.shard_map(device_step, mesh=mesh,
                         in_specs=(rows_spec, P(), P(), P(), P("ep"), P("ep"), P("ep"), rows_spec, rows_spec, rows_spec),
                         out_specs=rows_spec, check_vma=False)
```

```python
import functools
import math

import jax
import jax.numpy as jnp
from jax import lax
from jax.experimental import pallas as pl
from jax.experimental.pallas import tpu as pltpu
from jax.sharding import PartitionSpec as P

LN_EPS = 1e-5
LANES = 128
SPLIT = 2
DEPTH = 3
MESH = pl.DeviceIdType.MESH


def quotient(value, by):
    return lax.div(value, jnp.int32(by))


def remainder(value, by):
    return lax.rem(value, jnp.int32(by))


def moe_kernel(sizes, hidden_ref, gamma_ref, beta_ref, router_ref, own_ref, choice_ref, first_ref, second_ref,
               out_ref, gathered,
               normed, total, gu_buf, wd_buf, row_buf, inner_buf, gate_table, gate_wide,
               ring_send, ring_recv, side_send, side_recv, pair_send, pair_recv, own_send, own_recv,
               row_sem, load_sem):
    ring, columns, capacity = sizes
    tokens, width = hidden_ref.shape
    ff = own_ref.shape[1]
    experts = gathered.shape[0]
    half = tokens // 2
    tile = tokens // 8
    turns = 2 * SPLIT
    part_rows = ff // (2 * turns)
    rounds = SPLIT * (ring - 1)
    dp = lax.axis_index("dp")
    ep = lax.axis_index("ep")
    z, core = quotient(ep, 2), remainder(ep, 2)
    x, y = quotient(dp, columns), remainder(dp, columns)
    parity = remainder(x + y, 2)
    after, before = remainder(z + 1, ring) * 2 + core, remainder(z + ring - 1, ring) * 2 + core
    partner = z * 2 + 1 - core
    x_peer = (x + 1 - 2 * remainder(x, 2)) * columns + y
    y_peer = x * columns + y + 1 - 2 * remainder(y, 2)
    places = ((dp, after), (dp, before), (x_peer, ep), (y_peer, ep), (dp, partner))

    barrier = pltpu.get_barrier_semaphore()
    for place in places:
        pl.semaphore_signal(barrier, inc=1, device_id=place, device_id_type=MESH)
    pl.semaphore_wait(barrier, len(places))

    def piece(expert, part, own=False):
        rows = pl.ds(pl.multiple_of(part * part_rows, 8), part_rows)
        target = gathered.at[expert, :, rows, :]
        return (own_ref.at[:, rows, :] if own else target), target

    def copies(both, send, recv, place):
        return [pltpu.make_async_remote_copy(src_ref=both[0], dst_ref=both[1], send_sem=send, recv_sem=recv,
                                             device_id=place, device_id_type=MESH)]

    def ring_part(flow, index):
        return remainder(index + SPLIT * flow, turns)

    def far(flow, hops):
        return remainder(z + hops * (2 * flow - 1) + ring, ring) * 2

    def ring_copy(flow, index, own):
        both = piece(far(flow, quotient(index, turns)) + core, turns * parity + ring_part(flow, index), own)
        return copies(both, ring_send.at[flow, index], ring_recv.at[flow, index], places[flow])

    def came(flow, index, of_core, of_parity):
        return piece(far(flow, 1 + quotient(index, turns)) + of_core, turns * of_parity + ring_part(flow, index))

    def ring_arrival(flow, index):
        return copies(came(flow, index, core, parity), ring_send.at[flow, index], ring_recv.at[flow, index], places[flow])

    def carried(flow, index):
        return remainder(quotient(index, SPLIT) + flow, 2)

    def side_copy(flow, index, of_parity):
        return copies(came(carried(flow, index), index, core, of_parity), side_send.at[flow, index],
                      side_recv.at[flow, index], places[2 + flow])

    def pair_copy(flow, index, of_core):
        if flow < 2:
            both = came(flow, index, of_core, parity)
        else:
            both = came(carried(flow, index), index, of_core, 1 - parity)
        return copies(both, pair_send.at[flow, index], pair_recv.at[flow, index], places[4])

    def own_copy(expert):
        return copies((own_ref, gathered.at[expert]), own_send.at[0], own_recv.at[0], places[4])

    def start(group):
        for copy in group:
            copy.start()

    def wait_recv(group):
        for copy in group:
            copy.wait_recv()

    def wait_send(group):
        for copy in group:
            copy.wait_send()

    def row_load(index):
        rows = pl.ds(pl.multiple_of(index * tile, tile), tile)
        slot = remainder(index, 4)
        return pltpu.make_async_copy(hidden_ref.at[rows, :], row_buf.at[slot], row_sem.at[slot])

    def expert_of(turn):
        high, low = quotient(remainder(turn + 2, 4), 2), remainder(turn, 2)
        edge = (turn < 2) | (turn >= experts - 2)
        kind = jnp.where(edge, low, high)
        return far(jnp.where(edge, high, low), quotient(turn + 2, 4)) + core + kind * (1 - 2 * core)

    full, rest = ff // LANES, ff % LANES

    def loads(source, slot):
        made = [pltpu.make_async_copy(source.at[2], wd_buf.at[slot, pl.ds(0, ff), :], load_sem.at[slot, 0])]
        for index in range(full + 1):
            count = LANES if index < full else rest
            for kind in range(2):
                made.append(pltpu.make_async_copy(
                    source.at[kind, pl.ds(index * LANES, count), :],
                    gu_buf.at[slot, pl.ds(index * 2 * LANES + kind * count, count), :],
                    load_sem.at[slot, 1 + 2 * index + kind]))
        return made

    def expert_loads(turn):
        return loads(gathered.at[expert_of(turn)], remainder(turn, 2))

    start(loads(own_ref, 0))
    for index in range(4):
        row_load(index).start()
    for index in range(DEPTH):
        for flow in range(2):
            start(ring_copy(flow, index, True))
    start(own_copy(ep))
    padded = wd_buf.shape[1]
    wd_buf[:, pl.ds(ff, padded - ff), :] = jnp.zeros((2, padded - ff, width), wd_buf.dtype)

    def norm_tile(index):
        row_load(index).wait()
        rows = pl.ds(pl.multiple_of(index * tile, tile), tile)
        values = row_buf[remainder(index, 4)].astype(jnp.float32)
        total[rows, :] = values
        centred = values - jnp.mean(values, axis=-1, keepdims=True)
        variance = jnp.mean(centred * centred, axis=-1, keepdims=True)
        normed[rows, :] = (centred * lax.rsqrt(variance + LN_EPS) * gamma_ref[...] + beta_ref[...]).astype(jnp.bfloat16)

        @pl.when(index + 4 < 8)
        def _():
            row_load(index + 4).start()

    def hits(rows, pick, count):
        ids = lax.broadcasted_iota(jnp.int32, (experts, count), 0)
        return ids == choice_ref[pl.ds(pick, 1), rows]

    def gate_tile(index):
        step = 2 * tile
        rows = pl.ds(pl.multiple_of(index * step, step), step)
        scores = lax.dot_general(normed[rows, :], router_ref[...], (((1,), (1,)), ((), ())),
                                 preferred_element_type=jnp.float32)
        every = pl.ds(0, tokens)
        per_token = sum(jnp.where(hits(every, pick, tokens), 1.0, 0.0) for pick in range(2)).astype(jnp.bfloat16)
        earlier = (lax.broadcasted_iota(jnp.int32, (step, tokens), 1)
                   < lax.broadcasted_iota(jnp.int32, (step, tokens), 0) + index * step)
        position = lax.dot_general(jnp.where(earlier, 1.0, 0.0).astype(jnp.bfloat16), per_token, (((1,), (1,)), ((), ())),
                                   preferred_element_type=jnp.float32)
        table = jnp.full((step, experts), -1.0, jnp.float32)
        for pick, mask_ref in enumerate((first_ref, second_ref)):
            hit = jnp.where(hits(rows, pick, step), 1.0, 0.0).T > 0.0
            masked = jnp.where(mask_ref[:, rows].T > 0, scores, -jnp.inf)
            powers = jnp.exp(masked - jnp.max(masked, axis=-1, keepdims=True))
            probs = powers / jnp.sum(powers, axis=-1, keepdims=True)
            table = jnp.where(hit & (position < capacity), probs, table)
        gate_table[rows, :] = table

    def expert_unit(unit):
        turn, part = quotient(unit, 2), remainder(unit, 2)
        slot = remainder(turn, 2)
        expert = expert_of(turn)

        @pl.when(part == 0)
        def _():
            for copy in expert_loads(turn):
                copy.wait()

        @pl.when((part == 1) & (turn == 0))
        def _():
            wait_recv(own_copy(partner))

        @pl.when((part == 1) & (turn + 1 < experts))
        def _():
            start(expert_loads(turn + 1))

        rows = pl.ds(pl.multiple_of(part * half, half), half)
        ids = lax.broadcasted_iota(jnp.int32, (half, experts), 1)
        gates = jnp.sum(jnp.where(ids == expert, gate_table[rows, :], 0.0), axis=-1, keepdims=True)
        gate_wide[...] = jnp.broadcast_to(gates, gate_wide.shape)

        def project(outs):
            return lax.dot_general(normed[rows, :], gu_buf[slot, outs, :], (((1,), (1,)), ((), ())),
                                   preferred_element_type=jnp.float32)

        def inner_tile(index, _):
            both = project(pl.ds(pl.multiple_of(index * 2 * LANES, 2 * LANES), 2 * LANES))
            value = jax.nn.silu(both[:, :LANES]) * both[:, LANES:]
            inner_buf[:, pl.ds(pl.multiple_of(index * LANES, LANES), LANES)] = value.astype(jnp.bfloat16)
            return 0

        lax.fori_loop(0, full, inner_tile, 0)
        both = project(pl.ds(full * 2 * LANES, 2 * rest))
        value = jax.nn.silu(both) * pltpu.roll(both, LANES - rest, 1)
        lane = lax.broadcasted_iota(jnp.int32, value.shape, 1)
        inner_buf[:, pl.ds(full * LANES, LANES)] = jnp.where(lane < rest, value, 0.0).astype(jnp.bfloat16)

        step = min(width, 2 * LANES)

        def out_tile(index, _):
            lanes = pl.ds(pl.multiple_of(index * step, step), step)
            made = jnp.dot(inner_buf[...], wd_buf[slot, :, lanes], preferred_element_type=jnp.float32)
            made = made.astype(jnp.bfloat16).astype(jnp.float32)
            gate = jnp.concatenate([gate_wide[...]] * (step // LANES), axis=1) if step > LANES else gate_wide[:, :step]
            total[rows, lanes] += jnp.where(gate >= 0.0, gate * made, 0.0)
            return 0

        lax.fori_loop(0, width // step, out_tile, 0)

    last = rounds - 2

    def begin(step):
        late = jnp.where(step == last, 2 * experts - 13, jnp.where(step == last + 1, 2 * experts - 9, 2 * experts - 5))
        late = jnp.where(step < last + 3, late, jnp.where(step == last + 3, 2 * experts - 4, 2 * experts))
        return jnp.where(step < last, 2 * jnp.maximum(step - 3, 0), late)

    def step_body(step, _):
        @pl.when(step < rounds)
        def _():
            for flow in range(2):
                wait_recv(ring_arrival(flow, step))
            ahead = step + DEPTH
            for flow in range(2):
                @pl.when(ahead < turns)
                def _():
                    start(ring_copy(flow, ahead, True))

                @pl.when((ahead >= turns) & (ahead < rounds))
                def _():
                    start(ring_copy(flow, ahead, False))
            for flow in range(2):
                start(side_copy(flow, step, parity))
            for flow in range(2):
                start(pair_copy(flow, step, core))

        @pl.when((step >= 1) & (step <= rounds))
        def _():
            for flow in range(2):
                wait_recv(side_copy(flow, step - 1, 1 - parity))
            for flow in range(2):
                start(pair_copy(2 + flow, step - 1, core))

        @pl.when(step >= 2)
        def _():
            for flow in range(4):
                wait_recv(pair_copy(flow, step - 2, 1 - core))

        @pl.when(step < 2)
        def _():
            lax.fori_loop(4 * step, 4 * step + 4, lambda index, _: (norm_tile(index), 0)[1], 0)

        @pl.when(step == 1)
        def _():
            lax.fori_loop(0, 4, lambda index, _: (gate_tile(index), 0)[1], 0)

        lax.fori_loop(begin(step), begin(step + 1), lambda unit, _: (expert_unit(unit), 0)[1], 0)
        return 0

    lax.fori_loop(0, rounds + 2, step_body, 0)

    def row_store(index):
        rows = pl.ds(pl.multiple_of(index * tile, tile), tile)
        slot = remainder(index, 4)
        return pltpu.make_async_copy(row_buf.at[slot], out_ref.at[rows, :], row_sem.at[slot])

    def store_tile(index, _):
        @pl.when(index >= 4)
        def _():
            row_store(index - 4).wait()
        rows = pl.ds(pl.multiple_of(index * tile, tile), tile)
        row_buf[remainder(index, 4)] = total[rows, :].astype(row_buf.dtype)
        row_store(index).start()
        return 0

    lax.fori_loop(0, 8, store_tile, 0)
    for index in range(4, 8):
        row_store(index).wait()

    def finish(index, _):
        for flow in range(2):
            wait_send(ring_copy(flow, index, False))
            wait_send(side_copy(flow, index, parity))
        for flow in range(4):
            wait_send(pair_copy(flow, index, core))
        return 0

    lax.fori_loop(0, rounds, finish, 0)
    wait_send(own_copy(ep))


def solution(mesh):
    group_size = mesh.shape["ep"]
    columns = math.isqrt(mesh.shape["dp"])
    rows_spec = P(("dp", "ep"))

    def device_step(hidden, ln_gamma, ln_beta, w_router, w_gate, w_up, w_down, choice, mask_first, mask_second):
        tokens, width = hidden.shape
        experts = w_gate.shape[0] * group_size
        ff = w_gate.shape[2]
        capacity = (10 * tokens + 4 * experts - 1) // (4 * experts)
        ring = group_size // 2
        rounds = SPLIT * (ring - 1)
        padded = -(-ff // LANES) * LANES
        own = jnp.stack([w_gate[0].T, w_up[0].T, w_down[0]])
        dma = pltpu.SemaphoreType.DMA
        whole = pl.BlockSpec(memory_space=pl.ANY)
        local = pl.BlockSpec(memory_space=pltpu.VMEM)
        out, _ = pl.pallas_call(
            functools.partial(moe_kernel, (ring, columns, capacity)),
            out_shape=(jax.ShapeDtypeStruct(hidden.shape, hidden.dtype),
                       jax.ShapeDtypeStruct((experts, 3, ff, width), w_down.dtype)),
            in_specs=[whole, local, local, local, whole, local, local, local],
            out_specs=(whole, whole),
            scratch_shapes=[
                pltpu.VMEM((tokens, width), jnp.bfloat16),
                pltpu.VMEM((tokens, width), jnp.float32),
                pltpu.VMEM((2, 2 * ff, width), w_gate.dtype),
                pltpu.VMEM((2, padded, width), w_down.dtype),
                pltpu.VMEM((4, tokens // 8, width), hidden.dtype),
                pltpu.VMEM((tokens // 2, padded), jnp.bfloat16),
                pltpu.VMEM((tokens, experts), jnp.float32),
                pltpu.VMEM((tokens // 2, LANES), jnp.float32),
                dma((2, rounds)), dma((2, rounds)),
                dma((2, rounds)), dma((2, rounds)),
                dma((4, rounds)), dma((4, rounds)),
                dma((1,)), dma((1,)),
                dma((4,)), dma((2, 1 + 2 * (padded // LANES))),
            ],
            compiler_params=pltpu.CompilerParams(collective_id=0, has_side_effects=True, vmem_limit_bytes=67043328),
            name="moe",
        )(hidden, ln_gamma.reshape(1, width), ln_beta.reshape(1, width), w_router.T, own,
          choice.T, mask_first.T, mask_second.T)
        return out

    return jax.shard_map(device_step, mesh=mesh,
                         in_specs=(rows_spec, P(), P(), P(), P("ep"), P("ep"), P("ep"), rows_spec, rows_spec, rows_spec),
                         out_specs=rows_spec, check_vma=False)
```
